512 devices in a mesh: wall: 128 (over z, y, core), span: 4 (over x).
Axes of the slice: x: 4, y: 8, z: 8, core: 2. Of those that a mesh axis runs over, the one named last changes fastest.
Arguments:
- random_planes: float32 [8, 3, 2048, 4096], P(None, None, 'wall', 'span'), may hold values from -6 to 6
- previous: float32 [3, 2048, 4096], P(None, 'wall', 'span'), may hold values from -6 to 6
- half_width: int32 [2048], P('wall'), may hold values from 1 to 32
- time_scale: float32 [3, 2048], P(None, 'wall'), may hold values from 1 to 16
- lund_factor: float32 [6, 2048], P(None, 'wall'), may hold values from -4 to 4
- mean_velocity: float32 [2048], P('wall'), may hold values from 0.5 to 1.5
Outputs:
- velocity: float32 [8, 3, 2048, 4096], P(None, None, 'wall', 'span')
- filter_state: float32 [3, 2048, 4096], P(None, 'wall', 'span')
The draws below stay inside these ranges and needn't reach their ends.
All inputs are finite; a program needn't handle non-finite values.
Results may differ from the reference program's by a relative error of at most 0.000064.
Values sent between devices are 32-bit elements; how exact they have to be, the bound alone decides.
No kernel may reach another device: no remote copies, remote signals or barrier semaphores. Data moves between devices by JAX's collectives and lax.ppermute only.
A program may use at most 128 MiB of HBM per device.

```python
import math
import jax
import jax.numpy as jnp
from jax import lax

STEPS = 8
HMAX = 32
HZ = 24
NY = 2048
NZ = 4096


def set_ends(values, own_key, smallest, largest):
    index_at = [jax.random.randint(jax.random.fold_in(own_key, axis), (), 0, length) for axis, length in enumerate(values.shape)]
    longest = values.shape.index(max(values.shape))
    beside = index_at[:longest] + [(index_at[longest] + 1) % values.shape[longest]] + index_at[longest + 1:]
    return values.at[tuple(index_at)].set(smallest).at[tuple(beside)].set(largest)


def steps_of(rng, dims, split, low, largest):
    loudness, own = 1.0, jax.random.fold_in(rng, 6)
    for position, blocks in split:
        heights = jnp.exp(jax.random.uniform(jax.random.fold_in(own, position), (blocks,), jnp.float32, low / len(split), largest / len(split)))
        loudness = loudness * jnp.repeat(heights, dims[position] // blocks).reshape([-1 if axis == position else 1 for axis in range(len(dims))])
    return loudness


def centred(stream_key, extent, scale, most, pieces=(), kind=jnp.bfloat16):
    array = jax.random.normal(stream_key, extent, jnp.float32) * scale
    if len(pieces) > 0:
        array = steps_of(stream_key, extent, pieces, -0.22, 0.18) * array
    return jnp.clip(array, min=-most, max=most).astype(kind)


def setup_inputs(seed: int = 0) -> dict:
    keys = jax.random.split(jax.random.key(seed), 7)
    return {
        "random_planes": centred(keys[0], (STEPS, 3, NY, NZ), 1.0, 6.0, ((2, 128), (3, 4)), jnp.float32),
        "previous": centred(keys[1], (3, NY, NZ), 1.0, 6.0, ((1, 128), (2, 4)), jnp.float32),
        "half_width": set_ends(jax.random.randint(keys[2], (NY,), 1, HMAX + 1), jax.random.fold_in(keys[2], 1), 1, HMAX).astype(jnp.int32),
        "time_scale": jnp.clip(jnp.exp(math.log(16.0) - 2.7725887 * jax.random.uniform(keys[3], (3, NY), jnp.float32) ** steps_of(keys[3], (3, NY), ((1, 128),), -0.2, 0.2)), 1.0, 16.0),
        "lund_factor": centred(keys[4], (6, NY), 1.0, 4.0, ((1, 128),), jnp.float32),
        "mean_velocity": jnp.clip(0.5 + 1.0 * jax.random.uniform(keys[5], (NY,), jnp.float32) ** steps_of(keys[5], (NY,), ((0, 128),), -0.2, 0.2), 0.5, 1.5),
    }


def unit_weights(widths, reach):
    offsets = jnp.arange(-reach, reach + 1, dtype=jnp.int32)
    spread = widths.astype(jnp.float32)[:, None]
    distance = offsets.astype(jnp.float32)[None, :]
    shaped = jnp.where(jnp.abs(offsets)[None, :] <= widths[:, None], jnp.exp(-2.0 * math.pi * distance * distance / (spread * spread)), 0.0)
    return shaped / jnp.sqrt(lax.optimization_barrier(jnp.sum(shaped * shaped, axis=1, keepdims=True)))

def reference(random_planes, previous, half_width, time_scale, lund_factor, mean_velocity):
    wall_weights = unit_weights(half_width, HMAX)
    span_weights = unit_weights(jnp.full((1,), HZ, jnp.int32), HZ)[0]
    retain = jnp.exp(-math.pi / (2.0 * time_scale))[:, :, None]
    inject = jnp.sqrt(1.0 - jnp.exp(-math.pi / time_scale))[:, :, None]
    factor = lund_factor[:, :, None]

    def one_step(current, plane):
        padded = jnp.pad(plane, ((0, 0), (HMAX, HMAX), (0, 0)))

        def add_wall(offset, total):
            start = offset.astype(jnp.int32)
            rows = lax.dynamic_slice_in_dim(padded, start, NY, 1)
            weight = lax.dynamic_slice_in_dim(wall_weights, start, 1, 1)
            return total + weight[None, :, :] * rows
        wall_pass = lax.fori_loop(0, 2 * HMAX + 1, add_wall, jnp.zeros_like(plane))
        wrapped = jnp.concatenate([wall_pass[:, :, NZ - HZ:], wall_pass, wall_pass[:, :, :HZ]], axis=2)

        def add_span(offset, total):
            start = offset.astype(jnp.int32)
            cells = lax.dynamic_slice_in_dim(wrapped, start, NZ, 2)
            weight = lax.dynamic_index_in_dim(span_weights, start, 0, keepdims=False)
            return total + weight * cells
        filtered = lax.fori_loop(0, 2 * HZ + 1, add_span, jnp.zeros_like(plane))
        current = retain * current + inject * filtered
        stream = mean_velocity[:, None] + factor[0] * current[0]
        normal = factor[1] * current[0] + factor[2] * current[1]
        spanwise = factor[3] * current[0] + factor[4] * current[1] + factor[5] * current[2]
        return (current, jnp.stack([stream, normal, spanwise]))
    final, velocities = lax.scan(one_step, previous, random_planes)
    return (velocities, final)
```

```python
import math

import jax
import jax.numpy as jnp
import numpy as np
from jax import lax
from jax.experimental import pallas as pl
from jax.experimental.pallas import tpu as pltpu
from jax.sharding import PartitionSpec as P


HMAX = 32
HZ = 24
LANES = 128
TILE = 256
EDGE = 32
VMEM_BYTES = 16 * 2**20

f32 = jnp.float32
bf16 = jnp.bfloat16


def span_band():
    offsets = np.arange(-HZ, HZ + 1, dtype=np.float64)
    raw = np.exp(-2.0 * np.pi * offsets**2 / HZ**2)
    unit = raw / np.sqrt(np.sum(raw * raw))
    rows = np.arange(TILE + 2 * LANES)[:, None]
    cols = np.arange(TILE)[None, :]
    j = rows - LANES - cols
    band = np.where(np.abs(j) <= HZ, unit[np.clip(j + HZ, 0, 2 * HZ)], 0.0).astype(np.float32)
    high = band.astype(jnp.bfloat16)
    low = (band - high.astype(np.float32)).astype(jnp.bfloat16)
    return np.stack([high, low])


def halves(x):
    high = x.astype(bf16)
    return high, (x - high.astype(f32)).astype(bf16)


def dot(a, b):
    return jnp.dot(a, b, preferred_element_type=f32)


def spread(packed, last):
    pieces = []
    for group in range(LANES // EDGE):
        shift = (LANES - EDGE if last else 0) - group * EDGE
        pieces.append(pltpu.roll(packed, shift % LANES, 1) if shift else packed)
    return jnp.concatenate(pieces, axis=0)


def gathered(edge, last):
    count = edge.shape[0] // (LANES // EDGE)
    lane = lax.broadcasted_iota(jnp.int32, (count, LANES), 1) // EDGE
    total = jnp.zeros((count, LANES), f32)
    for group in range(LANES // EDGE):
        piece = edge[group * count : (group + 1) * count]
        shift = group * EDGE - (LANES - EDGE if last else 0)
        total = jnp.where(lane == group, pltpu.roll(piece, shift % LANES, 1) if shift else piece, total)
    return total


def pack_kernel(first_ref, last_ref, right_ref, left_ref):
    right_ref[...] = gathered(first_ref[...], False)
    left_ref[...] = gathered(last_ref[...], True)


def fill_window(x_ref, left, right, high_ref, low_ref):
    width = x_ref.shape[1]
    high_ref[:, :LANES], low_ref[:, :LANES] = halves(spread(left, True))
    high_ref[:, LANES : LANES + width], low_ref[:, LANES : LANES + width] = halves(x_ref[...])
    high_ref[:, LANES + width :], low_ref[:, LANES + width :] = halves(spread(right, False))


def span_filter(high_ref, low_ref, band_ref, store):
    width = high_ref.shape[1] - 2 * LANES
    for start in range(0, width, TILE):
        window = pl.ds(start, TILE + 2 * LANES)
        high = high_ref[:, window]
        low = low_ref[:, window]
        store(
            pl.ds(start, TILE),
            dot(high, band_ref[0]) + dot(low, band_ref[0]) + dot(high, band_ref[1]),
        )


def own_kernel(x_ref, left_ref, right_ref, band_ref, out_ref, edge_ref, high_ref, low_ref):
    fill_window(x_ref, left_ref[...], right_ref[...], high_ref, low_ref)
    count = left_ref.shape[0]
    edge_ref[:count, :] = left_ref[...]
    edge_ref[count:, :] = right_ref[...]

    def store(columns, value):
        out_ref[:, columns] = value

    span_filter(high_ref, low_ref, band_ref, store)


def wall_kernel(
    own_ref, far_ref, edge_ref, band_ref, weight_ref, mine_ref, theirs_ref,
    high_ref, low_ref, far_high_ref, far_low_ref,
):
    count = edge_ref.shape[0] // 2
    fill_window(far_ref, edge_ref[:count, :], edge_ref[count:, :], high_ref, low_ref)

    def store(columns, value):
        far_high_ref[:, columns], far_low_ref[:, columns] = halves(value)

    span_filter(high_ref, low_ref, band_ref, store)
    rows = weight_ref.shape[0] // 2
    planes = own_ref.shape[0] // rows
    group = 6

    def some_planes(index, carry):
        for one in range(group):
            at = pl.ds(pl.multiple_of((index * group + one) * rows, rows), rows)
            own_high, own_low = halves(own_ref[at, :])
            high = [own_high, far_high_ref[at, :]]
            low = [own_low, far_low_ref[at, :]]
            both = dot(weight_ref[...], jnp.concatenate(high + low + high, axis=0))
            mine_ref[at, :] = both[:rows]
            theirs_ref[at, :] = both[rows:]
        return carry

    lax.fori_loop(0, planes // group, some_planes, 0)


def step_kernel(
    mine_ref, theirs_ref, near_ref, weight_ref, row_ref, previous_ref, velocity_ref, state_ref,
    made_ref, field_ref, sems,
):
    rows = weight_ref.shape[0]
    repeat = previous_ref.shape[1] // LANES
    steps = made_ref.shape[0] // (3 * rows)

    def row(index):
        return jnp.concatenate([row_ref[index]] * repeat, axis=1)

    copies = []
    for step in range(steps):
        field = []
        for part in range(3):
            at = pl.ds((step * 3 + part) * rows, rows)
            of = pl.ds(part * rows, rows)
            high, low = halves(near_ref[at, :])
            total = mine_ref[at, :] + theirs_ref[at, :]
            total = total + dot(weight_ref[...], jnp.concatenate([high, low, high], axis=0))
            before = previous_ref[of, :] if step == 0 else field_ref[of, :]
            now = row(part) * before + row(3 + part) * total
            field_ref[of, :] = now
            field.append(now)
        at = step * 3 * rows
        made_ref[pl.ds(at, rows), :] = row(12) + row(6) * field[0]
        made_ref[pl.ds(at + rows, rows), :] = row(7) * field[0] + row(8) * field[1]
        made_ref[pl.ds(at + 2 * rows, rows), :] = (
            row(9) * field[0] + row(10) * field[1] + row(11) * field[2]
        )
        block = pl.ds(at, 3 * rows)
        copy = pltpu.make_async_copy(made_ref.at[block], velocity_ref.at[block], sems.at[step])
        copy.start()
        copies.append(copy)
    copy = pltpu.make_async_copy(field_ref, state_ref, sems.at[steps])
    copy.start()
    for one in copies + [copy]:
        one.wait()


WHOLE = pl.BlockSpec(memory_space=pltpu.VMEM)


def vmem(x):
    return pltpu.with_memory_space_constraint(x, pltpu.VMEM)


def hbm(x):
    return pltpu.with_memory_space_constraint(x, pltpu.HBM)


def call(kernel, out, scratch, flops, *args, in_specs=None, out_specs=WHOLE, **more):
    moved = sum(a.size * a.dtype.itemsize for a in args)
    return pl.pallas_call(
        kernel,
        out_shape=out,
        in_specs=in_specs or [WHOLE] * len(args),
        out_specs=jax.tree.map(lambda _: out_specs, out),
        scratch_shapes=scratch,
        cost_estimate=pl.CostEstimate(flops=flops, bytes_accessed=moved, transcendentals=0),
        compiler_params=pltpu.CompilerParams(vmem_limit_bytes=VMEM_BYTES),
        **more,
    )(*args)


def wall_weights(widths, *starts):
    count = widths.shape[0]
    spread = widths.astype(f32)[:, None]

    def raw(offset):
        distance = offset.astype(f32)
        return jnp.where(
            jnp.abs(offset) <= widths[:, None],
            jnp.exp(-2.0 * math.pi * distance * distance / (spread * spread)),
            0.0,
        )

    every = raw(lax.broadcasted_iota(jnp.int32, (count, 2 * HMAX + 1), 1) - HMAX)
    size = jnp.sqrt(jnp.sum(every * every, axis=1, keepdims=True))
    row = lax.broadcasted_iota(jnp.int32, (count, count), 0)
    col = lax.broadcasted_iota(jnp.int32, (count, count), 1)
    return [raw(col - row + start) / size for start in starts]


def split3(weights):
    high = lax.reduce_precision(weights, exponent_bits=8, mantissa_bits=7)
    low = lax.reduce_precision(weights - high, exponent_bits=8, mantissa_bits=7)
    return jnp.concatenate([high, high, low], axis=1).astype(bf16)


def planes(random_planes, previous, half_width, time_scale, lund_factor, mean_velocity):
    steps, parts, rows, width = random_planes.shape
    wall = lax.axis_size("wall")
    span = lax.axis_size("span")
    core = lax.axis_index("wall") % 2
    sign = 1 - 2 * core
    near_pairs = []
    far_pairs = []
    for at in range(wall):
        way = 2 - 4 * (at % 2)
        if 0 <= at - way < wall:
            near_pairs.append((at - way, at))
        if 0 <= at + way < wall:
            far_pairs.append((at + way, at))
    swap = [(at, at ^ 1) for at in range(wall)]
    forward = [(i, (i + 1) % span) for i in range(span)]
    backward = [(target, source) for source, target in forward]

    x = random_planes.reshape(steps * parts * rows, width)
    count = x.shape[0]
    packed_rows = count * EDGE // LANES
    far = lax.ppermute(x, "wall", far_pairs)
    packed = pltpu.VMEM((packed_rows, LANES), f32)
    mine_right, mine_left = call(
        pack_kernel, (packed, packed), [], 0, hbm(x), hbm(x),
        in_specs=[
            pl.BlockSpec((count, LANES), lambda i: (0, 0)),
            pl.BlockSpec((count, LANES), lambda i: (0, width // LANES - 1)),
        ],
        grid=(1,),
    )
    left = lax.ppermute(mine_left, "span", forward)
    right = lax.ppermute(mine_right, "span", backward)

    band = jnp.asarray(span_band())
    block = pltpu.VMEM(x.shape, f32)
    window = pltpu.VMEM((count, width + 2 * LANES), bf16)
    inner = pltpu.VMEM((count, width), bf16)
    span_flops = 2 * count * width * 512 * 3
    wall_flops = 2 * count * width * 32 * 6
    own, far_edges = call(
        own_kernel, (block, pltpu.VMEM((2 * packed_rows, LANES), f32)), [window] * 2,
        span_flops, vmem(x), vmem(left), vmem(right), vmem(band),
    )
    near = lax.ppermute(own, "wall", near_pairs)
    far_edges = lax.ppermute(far_edges, "wall", far_pairs)
    other_width = lax.ppermute(half_width, "wall", swap)

    own_w, far_w, near_w = wall_weights(half_width, 0, 2 * rows * sign, -2 * rows * sign)
    own_o, far_o = wall_weights(other_width, -rows * sign, rows * sign)
    both = split3(jnp.concatenate(
        [jnp.concatenate([own_w, far_w], axis=1), jnp.concatenate([own_o, far_o], axis=1)],
        axis=0,
    ))
    near_w = split3(near_w)
    retain = jnp.exp(-math.pi / (2.0 * time_scale))
    inject = jnp.sqrt(1.0 - jnp.exp(-math.pi / time_scale))
    per_row = jnp.concatenate([retain, inject, lund_factor, mean_velocity[None]], axis=0)
    per_row = jnp.broadcast_to(per_row[:, :, None], per_row.shape + (LANES,))
    mine, theirs = call(
        wall_kernel, (block, block), [window] * 2 + [inner] * 2,
        span_flops + wall_flops, vmem(own), vmem(far), vmem(far_edges), vmem(band), vmem(both),
    )
    theirs = lax.ppermute(theirs, "wall", swap)
    velocity, state = call(
        step_kernel,
        (jax.ShapeDtypeStruct(x.shape, f32), jax.ShapeDtypeStruct((parts * rows, width), f32)),
        [
            pltpu.VMEM(x.shape, f32), pltpu.VMEM((parts * rows, width), f32),
            pltpu.SemaphoreType.DMA((steps + 1,)),
        ],
        wall_flops, vmem(mine), vmem(theirs), vmem(near), vmem(near_w), vmem(per_row),
        vmem(previous.reshape(parts * rows, width)),
        out_specs=pl.BlockSpec(memory_space=pl.ANY),
    )
    return velocity.reshape(random_planes.shape), state.reshape(previous.shape)


def solution(mesh):
    in_specs = (
        P(None, None, "wall", "span"),
        P(None, "wall", "span"),
        P("wall"),
        P(None, "wall"),
        P(None, "wall"),
        P("wall"),
    )
    out_specs = (P(None, None, "wall", "span"), P(None, "wall", "span"))
    return jax.shard_map(planes, mesh=mesh, in_specs=in_specs, out_specs=out_specs, check_vma=False)
```

```python
import math

import jax
import jax.numpy as jnp
import numpy as np
from jax import lax
from jax.experimental import pallas as pl
from jax.experimental.pallas import tpu as pltpu
from jax.sharding import PartitionSpec as P


HMAX = 32
HZ = 24
LANES = 128
TILE = 256
EDGE = 32
LAST_STEPS = 2
VMEM_BYTES = 16 * 2**20

f32 = jnp.float32
bf16 = jnp.bfloat16


def span_band():
    offsets = np.arange(-HZ, HZ + 1, dtype=np.float64)
    raw = np.exp(-2.0 * np.pi * offsets**2 / HZ**2)
    unit = raw / np.sqrt(np.sum(raw * raw))
    rows = np.arange(TILE + 2 * LANES)[:, None]
    cols = np.arange(TILE)[None, :]
    j = rows - LANES - cols
    band = np.where(np.abs(j) <= HZ, unit[np.clip(j + HZ, 0, 2 * HZ)], 0.0).astype(np.float32)
    high = band.astype(jnp.bfloat16)
    low = (band - high.astype(np.float32)).astype(jnp.bfloat16)
    return np.stack([high, low])


def halves(x):
    high = x.astype(bf16)
    return high, (x - high.astype(f32)).astype(bf16)


def dot(a, b):
    return jnp.dot(a, b, preferred_element_type=f32)


def spread(packed, last):
    pieces = []
    for group in range(LANES // EDGE):
        shift = (LANES - EDGE if last else 0) - group * EDGE
        pieces.append(pltpu.roll(packed, shift % LANES, 1) if shift else packed)
    return jnp.concatenate(pieces, axis=0)


def gathered(edge, last):
    count = edge.shape[0] // (LANES // EDGE)
    lane = lax.broadcasted_iota(jnp.int32, (count, LANES), 1) // EDGE
    total = jnp.zeros((count, LANES), f32)
    for group in range(LANES // EDGE):
        piece = edge[group * count : (group + 1) * count]
        shift = group * EDGE - (LANES - EDGE if last else 0)
        total = jnp.where(lane == group, pltpu.roll(piece, shift % LANES, 1) if shift else piece, total)
    return total


def pack_kernel(first_ref, last_ref, right_ref, left_ref):
    right_ref[...] = gathered(first_ref[...], False)
    left_ref[...] = gathered(last_ref[...], True)


def put(high_ref, low_ref, start, value):
    at = pl.ds(start, value.shape[1])
    high_ref[:, at], low_ref[:, at] = halves(value)


def fill_inner(x_ref, high_ref, low_ref):
    width = x_ref.shape[1]
    put(high_ref, low_ref, 0, x_ref[:, TILE - LANES : width - TILE + LANES])


def fill_outer(x_ref, left, right, high_ref, low_ref):
    own = TILE + LANES
    put(high_ref, low_ref, 0, spread(left, True))
    put(high_ref, low_ref, LANES, x_ref[:, :own])
    put(high_ref, low_ref, LANES + own, x_ref[:, x_ref.shape[1] - own :])
    put(high_ref, low_ref, LANES + 2 * own, spread(right, False))


def filtered(high_ref, low_ref, band_ref, start):
    window = pl.ds(start, TILE + 2 * LANES)
    high = high_ref[:, window]
    return (
        dot(high, band_ref[0]) + dot(low_ref[:, window], band_ref[0]) + dot(high, band_ref[1])
    )


def own_inner_kernel(x_ref, band_hbm, out_ref, band_ref, high_ref, low_ref, sem):
    copy = pltpu.make_async_copy(band_hbm, band_ref, sem)
    copy.start()
    fill_inner(x_ref, high_ref, low_ref)
    copy.wait()
    for at in range(TILE, x_ref.shape[1] - TILE, TILE):
        out_ref[:, at - TILE : at] = filtered(high_ref, low_ref, band_ref, at - TILE)


def own_outer_kernel(
    inner_ref, x_ref, left_ref, right_ref, band_ref, first_ref, last_ref, edge_ref,
    high_ref, low_ref,
):
    count = left_ref.shape[0]
    edge_ref[:count, :] = left_ref[...]
    edge_ref[count:, :] = right_ref[...]
    fill_outer(x_ref, left_ref[...], right_ref[...], high_ref, low_ref)
    split = first_ref.shape[0]
    end = x_ref.shape[1] - TILE
    first_ref[:, TILE:end] = inner_ref[:split, :]
    last_ref[:, TILE:end] = inner_ref[split:, :]
    for at, start in ((0, 0), (end, TILE + 2 * LANES)):
        value = filtered(high_ref, low_ref, band_ref, start)
        first_ref[:, at : at + TILE] = value[:split]
        last_ref[:, at : at + TILE] = value[split:]


def wall_sums(block_of, weight_ref, planes, store):
    rows = weight_ref.shape[0] // 2
    group = 6

    def some_planes(index, carry):
        for one in range(group):
            at = pl.ds(pl.multiple_of((index * group + one) * rows, rows), rows)
            high, low = block_of(at)
            both = dot(weight_ref[...], jnp.concatenate([high, low, high], axis=0))
            store(at, both[:rows], both[rows:])
        return carry

    lax.fori_loop(0, planes // group, some_planes, 0)


def own_sums_kernel(first_ref, last_ref, weight_ref, mine_ref, theirs_ref):
    rows = weight_ref.shape[0] // 2
    base = 0
    for own_ref in (first_ref, last_ref):

        def store(at, mine, theirs, base=base):
            to = pl.ds(pl.multiple_of(at.start + base, rows), rows)
            mine_ref[to, :] = mine
            theirs_ref[to, :] = theirs

        planes = own_ref.shape[0] // rows
        wall_sums(lambda at, own_ref=own_ref: halves(own_ref[at, :]), weight_ref, planes, store)
        base += own_ref.shape[0]


def far_sums_kernel(
    mine_own_ref, theirs_own_ref, far_ref, edge_ref, band_ref, weight_ref, mine_ref, theirs_ref,
    high_ref, low_ref, far_high_ref, far_low_ref,
):
    count = edge_ref.shape[0] // 2
    width = far_ref.shape[1]
    put(high_ref, low_ref, 0, spread(edge_ref[:count, :], True))
    put(high_ref, low_ref, LANES, far_ref[...])
    put(high_ref, low_ref, LANES + width, spread(edge_ref[count:, :], False))
    for at in range(0, width, TILE):
        put(far_high_ref, far_low_ref, at, filtered(high_ref, low_ref, band_ref, at))

    def store(at, mine, theirs):
        mine_ref[at, :] = mine_own_ref[at, :] + mine
        theirs_ref[at, :] = theirs_own_ref[at, :] + theirs

    planes = far_ref.shape[0] * 2 // weight_ref.shape[0]
    wall_sums(lambda at: (far_high_ref[at, :], far_low_ref[at, :]), weight_ref, planes, store)


def some_steps(
    base, mine_ref, theirs_ref, near_ref, weight_ref, row_ref, before_ref, velocity_ref,
    made_ref, field_ref, sems,
):
    rows = weight_ref.shape[0]
    repeat = near_ref.shape[1] // LANES

    def row(index):
        return jnp.concatenate([row_ref[index]] * repeat, axis=1)

    copies = []
    for step in range(near_ref.shape[0] // (3 * rows)):
        field = []
        for part in range(3):
            at = (step * 3 + part) * rows
            of = pl.ds(part * rows, rows)
            high, low = halves(near_ref[pl.ds(at, rows), :])
            total = mine_ref[pl.ds(base + at, rows), :] + theirs_ref[pl.ds(base + at, rows), :]
            total = total + dot(weight_ref[...], jnp.concatenate([high, low, high], axis=0))
            before = before_ref[of, :] if step == 0 else field_ref[of, :]
            now = row(part) * before + row(3 + part) * total
            field_ref[of, :] = now
            field.append(now)
        at = step * 3 * rows
        made_ref[pl.ds(at, rows), :] = row(12) + row(6) * field[0]
        made_ref[pl.ds(at + rows, rows), :] = row(7) * field[0] + row(8) * field[1]
        made_ref[pl.ds(at + 2 * rows, rows), :] = (
            row(9) * field[0] + row(10) * field[1] + row(11) * field[2]
        )
        copy = pltpu.make_async_copy(
            made_ref.at[pl.ds(at, 3 * rows)], velocity_ref.at[pl.ds(base + at, 3 * rows)],
            sems.at[step],
        )
        copy.start()
        copies.append(copy)
    return copies


def first_steps_kernel(
    mine_ref, theirs_ref, near_ref, weight_ref, row_ref, before_ref, velocity_ref, field_ref,
    made_ref, sems,
):
    for copy in some_steps(
        0, mine_ref, theirs_ref, near_ref, weight_ref, row_ref, before_ref, velocity_ref,
        made_ref, field_ref, sems,
    ):
        copy.wait()


def last_steps_kernel(
    _, mine_ref, theirs_ref, near_ref, weight_ref, row_ref, before_ref, velocity_ref, state_ref,
    made_ref, field_ref, sems,
):
    copies = some_steps(
        mine_ref.shape[0] - near_ref.shape[0], mine_ref, theirs_ref, near_ref, weight_ref,
        row_ref, before_ref, velocity_ref, made_ref, field_ref, sems,
    )
    copy = pltpu.make_async_copy(field_ref, state_ref, sems.at[len(copies)])
    copy.start()
    for one in copies + [copy]:
        one.wait()


WHOLE = pl.BlockSpec(memory_space=pltpu.VMEM)


def vmem(x):
    return pltpu.with_memory_space_constraint(x, pltpu.VMEM)


def hbm(x):
    return pltpu.with_memory_space_constraint(x, pltpu.HBM)


def call(kernel, out, scratch, flops, *args, in_specs=None, out_specs=None, **more):
    moved = sum(a.size * a.dtype.itemsize for a in args)
    return pl.pallas_call(
        kernel,
        out_shape=out,
        in_specs=in_specs or [WHOLE] * len(args),
        out_specs=out_specs or jax.tree.map(lambda _: WHOLE, out),
        scratch_shapes=scratch,
        cost_estimate=pl.CostEstimate(flops=flops, bytes_accessed=moved, transcendentals=0),
        compiler_params=pltpu.CompilerParams(vmem_limit_bytes=VMEM_BYTES),
        **more,
    )(*args)


def of_rows(scalars, rows):
    row = lax.broadcasted_iota(jnp.int32, (rows, LANES), 0)
    total = jnp.full((rows, LANES), scalars[0])
    for index in range(1, rows):
        total = jnp.where(row == index, scalars[index], total)
    return total


def weight_kernel(
    width_ref, other_ref, scale_ref, factor_ref, mean_ref, own_ref, far_ref, near_ref, row_ref
):
    rows = width_ref.shape[0]
    sign = 1 - 2 * (lax.axis_index("wall") % 2)
    lane = lax.broadcasted_iota(jnp.int32, (rows, LANES), 1)
    row = lax.broadcasted_iota(jnp.int32, (rows, LANES), 0)

    def raw(widths, offset):
        spread = widths.astype(f32)
        distance = offset.astype(f32)
        return jnp.where(
            jnp.abs(offset) <= widths,
            jnp.exp(-2.0 * math.pi * distance * distance / (spread * spread)),
            0.0,
        )

    def unit(widths, start):
        every = raw(widths, lane - HMAX)
        size = jnp.sqrt(jnp.sum(every * every, axis=1, keepdims=True))
        return raw(widths, lane % rows - row + start) / size

    def three(weights):
        high, low = halves(weights)
        return jnp.where(lane < 2 * rows, high.astype(f32), low.astype(f32))[:, : 3 * rows].astype(bf16)

    mine = of_rows([width_ref[i] for i in range(rows)], rows)
    other = of_rows([other_ref[i] for i in range(rows)], rows)
    own_ref[:rows, :] = three(unit(mine, 0))
    own_ref[rows:, :] = three(unit(other, -rows * sign))
    far_ref[:rows, :] = three(unit(mine, 2 * rows * sign))
    far_ref[rows:, :] = three(unit(other, rows * sign))
    near_ref[...] = three(unit(mine, -2 * rows * sign))
    for part in range(3):
        scale = of_rows([scale_ref[part, i] for i in range(rows)], rows)
        row_ref[part] = jnp.exp(-math.pi / (2.0 * scale))
        row_ref[3 + part] = jnp.sqrt(1.0 - jnp.exp(-math.pi / scale))
    for entry in range(6):
        row_ref[6 + entry] = of_rows([factor_ref[entry, i] for i in range(rows)], rows)
    row_ref[12] = of_rows([mean_ref[i] for i in range(rows)], rows)


def planes(random_planes, previous, half_width, time_scale, lund_factor, mean_velocity):
    steps, parts, rows, width = random_planes.shape
    wall = lax.axis_size("wall")
    span = lax.axis_size("span")
    near_pairs = []
    far_pairs = []
    for at in range(wall):
        way = 2 - 4 * (at % 2)
        if 0 <= at - way < wall:
            near_pairs.append((at - way, at))
        if 0 <= at + way < wall:
            far_pairs.append((at + way, at))
    swap = [(at, at ^ 1) for at in range(wall)]
    forward = [(i, (i + 1) % span) for i in range(span)]
    backward = [(target, source) for source, target in forward]

    x = random_planes.reshape(steps * parts * rows, width)
    count = x.shape[0]
    packed_rows = count * EDGE // LANES
    far = lax.ppermute(x, "wall", far_pairs)
    packed = pltpu.VMEM((packed_rows, LANES), f32)
    mine_right, mine_left = call(
        pack_kernel, (packed, packed), [], 0, hbm(x), hbm(x),
        in_specs=[
            pl.BlockSpec((count, LANES), lambda i: (0, 0)),
            pl.BlockSpec((count, LANES), lambda i: (0, width // LANES - 1)),
        ],
        grid=(1,),
    )
    left = lax.ppermute(mine_left, "span", forward)
    right = lax.ppermute(mine_right, "span", backward)

    band = jnp.asarray(span_band())
    split = max(steps - LAST_STEPS, 1) * parts * rows
    block = pltpu.VMEM(x.shape, f32)
    part = pltpu.VMEM((count, width - 2 * TILE), f32)
    inner = [pltpu.VMEM((count, width - 2 * TILE + 2 * LANES), bf16)] * 2
    outer = [pltpu.VMEM((count, 2 * TILE + 4 * LANES), bf16)] * 2
    window = [pltpu.VMEM((count, width + 2 * LANES), bf16)] * 2
    far_parts = [pltpu.VMEM((count, width), bf16)] * 2
    span_flops = count * width * 512 * 3
    wall_flops = count * width * 32 * 6
    own, band = call(
        own_inner_kernel, (part, pltpu.VMEM(band.shape, bf16)),
        inner + [pltpu.SemaphoreType.DMA(())], span_flops, vmem(x), hbm(band),
        in_specs=[WHOLE, pl.BlockSpec(memory_space=pl.ANY)],
    )
    own_first, own_last, far_edges = call(
        own_outer_kernel,
        (
            pltpu.VMEM((split, width), f32), pltpu.VMEM((count - split, width), f32),
            pltpu.VMEM((2 * packed_rows, LANES), f32),
        ),
        outer, span_flops, vmem(own), vmem(x), vmem(left), vmem(right), vmem(band),
    )
    near_first = lax.ppermute(own_first, "wall", near_pairs)
    near_last = lax.ppermute(own_last, "wall", near_pairs)
    far_edges = lax.ppermute(far_edges, "wall", far_pairs)
    other_width = lax.ppermute(half_width, "wall", swap)

    scalars = pl.BlockSpec(memory_space=pltpu.SMEM)
    own_both, far_both, near_w, per_row = call(
        weight_kernel,
        (
            pltpu.VMEM((2 * rows, 3 * rows), bf16), pltpu.VMEM((2 * rows, 3 * rows), bf16),
            pltpu.VMEM((rows, 3 * rows), bf16), pltpu.VMEM((13, rows, LANES), f32),
        ),
        [], 0, half_width, other_width, time_scale, lund_factor, mean_velocity,
        in_specs=[scalars] * 5,
    )
    mine, theirs = call(
        own_sums_kernel, (block, block), [], wall_flops, vmem(own_first),
        vmem(own_last), vmem(own_both),
    )
    mine, theirs = call(
        far_sums_kernel, (block, block), window + far_parts,
        2 * span_flops + wall_flops, vmem(mine), vmem(theirs), vmem(far), vmem(far_edges),
        vmem(band), vmem(far_both),
    )
    theirs = lax.ppermute(theirs, "wall", swap)
    mine, theirs, near_w, per_row = vmem(mine), vmem(theirs), vmem(near_w), vmem(per_row)
    line = (parts * rows, width)
    anywhere = pl.BlockSpec(memory_space=pl.ANY)
    velocity, field = call(
        first_steps_kernel,
        (jax.ShapeDtypeStruct(x.shape, f32), pltpu.VMEM(line, f32)),
        [pltpu.VMEM((split, width), f32), pltpu.SemaphoreType.DMA((steps,))],
        wall_flops, mine, theirs, vmem(near_first), near_w, per_row,
        vmem(previous.reshape(line)), out_specs=(anywhere, WHOLE),
    )
    velocity, state = call(
        last_steps_kernel,
        (jax.ShapeDtypeStruct(x.shape, f32), jax.ShapeDtypeStruct(line, f32)),
        [
            pltpu.VMEM((count - split, width), f32), pltpu.VMEM(line, f32),
            pltpu.SemaphoreType.DMA((steps + 1,)),
        ],
        wall_flops, velocity, mine, theirs, vmem(near_last), near_w, per_row, vmem(field),
        in_specs=[anywhere] + [WHOLE] * 6, out_specs=(anywhere, anywhere),
        input_output_aliases={0: 0},
    )
    return velocity.reshape(random_planes.shape), state.reshape(previous.shape)


def solution(mesh):
    in_specs = (
        P(None, None, "wall", "span"),
        P(None, "wall", "span"),
        P("wall"),
        P(None, "wall"),
        P(None, "wall"),
        P("wall"),
    )
    out_specs = (P(None, None, "wall", "span"), P(None, "wall", "span"))
    return jax.shard_map(planes, mesh=mesh, in_specs=in_specs, out_specs=out_specs, check_vma=False)
```

```python
import math

import jax
import jax.numpy as jnp
import numpy as np
from jax import lax
from jax.experimental import pallas as pl
from jax.experimental.pallas import tpu as pltpu
from jax.sharding import PartitionSpec as P


HMAX = 32
HZ = 24
LANES = 128
TILE = 256
EDGE = 32
LAST_STEPS = 2
VMEM_BYTES = 16 * 2**20

f32 = jnp.float32
bf16 = jnp.bfloat16


def span_band():
    offsets = np.arange(-HZ, HZ + 1, dtype=np.float64)
    raw = np.exp(-2.0 * np.pi * offsets**2 / HZ**2)
    unit = raw / np.sqrt(np.sum(raw * raw))
    rows = np.arange(TILE + 2 * LANES)[:, None]
    cols = np.arange(TILE)[None, :]
    j = rows - LANES - cols
    band = np.where(np.abs(j) <= HZ, unit[np.clip(j + HZ, 0, 2 * HZ)], 0.0).astype(np.float32)
    high = band.astype(jnp.bfloat16)
    low = (band - high.astype(np.float32)).astype(jnp.bfloat16)
    return np.stack([high, low])


def halves(x):
    high = x.astype(bf16)
    return high, (x - high.astype(f32)).astype(bf16)


def dot(a, b):
    return jnp.dot(a, b, preferred_element_type=f32)


def spread(packed, last):
    pieces = []
    for group in range(LANES // EDGE):
        shift = (LANES - EDGE if last else 0) - group * EDGE
        pieces.append(pltpu.roll(packed, shift % LANES, 1) if shift else packed)
    return jnp.concatenate(pieces, axis=0)


def gathered(edge, last):
    count = edge.shape[0] // (LANES // EDGE)
    lane = lax.broadcasted_iota(jnp.int32, (count, LANES), 1) // EDGE
    total = jnp.zeros((count, LANES), f32)
    for group in range(LANES // EDGE):
        piece = edge[group * count : (group + 1) * count]
        shift = group * EDGE - (LANES - EDGE if last else 0)
        total = jnp.where(lane == group, pltpu.roll(piece, shift % LANES, 1) if shift else piece, total)
    return total


def pack_kernel(first_ref, last_ref, right_ref, left_ref):
    right_ref[...] = gathered(first_ref[...], False)
    left_ref[...] = gathered(last_ref[...], True)


def put(high_ref, low_ref, start, value):
    at = pl.ds(start, value.shape[1])
    high_ref[:, at], low_ref[:, at] = halves(value)


def fill_inner(x_ref, high_ref, low_ref):
    width = x_ref.shape[1]
    put(high_ref, low_ref, 0, x_ref[:, TILE - LANES : width - TILE + LANES])


def fill_outer(x_ref, left, right, high_ref, low_ref):
    own = TILE + LANES
    put(high_ref, low_ref, 0, spread(left, True))
    put(high_ref, low_ref, LANES, x_ref[:, :own])
    put(high_ref, low_ref, LANES + own, x_ref[:, x_ref.shape[1] - own :])
    put(high_ref, low_ref, LANES + 2 * own, spread(right, False))


def filtered(high_ref, low_ref, band_ref, start):
    window = pl.ds(start, TILE + 2 * LANES)
    high = high_ref[:, window]
    return (
        dot(high, band_ref[0]) + dot(low_ref[:, window], band_ref[0]) + dot(high, band_ref[1])
    )


def own_inner_kernel(x_ref, band_hbm, out_ref, band_ref, high_ref, low_ref, sem):
    copy = pltpu.make_async_copy(band_hbm, band_ref, sem)
    copy.start()
    fill_inner(x_ref, high_ref, low_ref)
    copy.wait()
    for at in range(TILE, x_ref.shape[1] - TILE, TILE):
        out_ref[:, at - TILE : at] = filtered(high_ref, low_ref, band_ref, at - TILE)


def own_outer_kernel(
    inner_ref, x_ref, left_ref, right_ref, band_ref, first_ref, last_ref, edge_ref,
    high_ref, low_ref,
):
    count = left_ref.shape[0]
    edge_ref[:count, :] = left_ref[...]
    edge_ref[count:, :] = right_ref[...]
    fill_outer(x_ref, left_ref[...], right_ref[...], high_ref, low_ref)
    split = first_ref.shape[0]
    end = x_ref.shape[1] - TILE
    first_ref[:, TILE:end] = inner_ref[:split, :]
    last_ref[:, TILE:end] = inner_ref[split:, :]
    for at, start in ((0, 0), (end, TILE + 2 * LANES)):
        value = filtered(high_ref, low_ref, band_ref, start)
        first_ref[:, at : at + TILE] = value[:split]
        last_ref[:, at : at + TILE] = value[split:]


def wall_sums(block_of, weight_ref, planes, store):
    rows = weight_ref.shape[0] // 2
    group = 6

    def some_planes(index, carry):
        for one in range(group):
            at = pl.ds(pl.multiple_of((index * group + one) * rows, rows), rows)
            high, low = block_of(at)
            both = dot(weight_ref[...], jnp.concatenate([high, low, high], axis=0))
            store(at, both[:rows], both[rows:])
        return carry

    lax.fori_loop(0, planes // group, some_planes, 0)


def own_sums_kernel(first_ref, last_ref, weight_ref, mine_ref, theirs_ref):
    rows = weight_ref.shape[0] // 2
    base = 0
    for own_ref in (first_ref, last_ref):

        def store(at, mine, theirs, base=base):
            to = pl.ds(pl.multiple_of(at.start + base, rows), rows)
            mine_ref[to, :] = mine
            theirs_ref[to, :] = theirs

        planes = own_ref.shape[0] // rows
        wall_sums(lambda at, own_ref=own_ref: halves(own_ref[at, :]), weight_ref, planes, store)
        base += own_ref.shape[0]


def far_sums_kernel(
    mine_own_ref, theirs_own_ref, far_ref, edge_ref, band_ref, weight_ref, mine_ref, theirs_ref,
    high_ref, low_ref, far_high_ref, far_low_ref,
):
    count = edge_ref.shape[0] // 2
    width = far_ref.shape[1]
    put(high_ref, low_ref, 0, spread(edge_ref[:count, :], True))
    put(high_ref, low_ref, LANES, far_ref[...])
    put(high_ref, low_ref, LANES + width, spread(edge_ref[count:, :], False))
    for at in range(0, width, TILE):
        put(far_high_ref, far_low_ref, at, filtered(high_ref, low_ref, band_ref, at))

    def store(at, mine, theirs):
        mine_ref[at, :] = mine_own_ref[at, :] + mine
        theirs_ref[at, :] = theirs_own_ref[at, :] + theirs

    planes = far_ref.shape[0] * 2 // weight_ref.shape[0]
    wall_sums(lambda at: (far_high_ref[at, :], far_low_ref[at, :]), weight_ref, planes, store)


def some_steps(
    base, mine_ref, theirs_ref, near_ref, weight_ref, row_ref, before_ref, velocity_ref,
    made_ref, field_ref, sems,
):
    rows = weight_ref.shape[0]
    repeat = near_ref.shape[1] // LANES

    def row(index):
        return jnp.concatenate([row_ref[index]] * repeat, axis=1)

    copies = []
    for step in range(near_ref.shape[0] // (3 * rows)):
        field = []
        for part in range(3):
            at = (step * 3 + part) * rows
            of = pl.ds(part * rows, rows)
            high, low = halves(near_ref[pl.ds(at, rows), :])
            total = mine_ref[pl.ds(base + at, rows), :] + theirs_ref[pl.ds(base + at, rows), :]
            total = total + dot(weight_ref[...], jnp.concatenate([high, low, high], axis=0))
            before = before_ref[of, :] if step == 0 else field_ref[of, :]
            now = row(part) * before + row(3 + part) * total
            field_ref[of, :] = now
            field.append(now)
        at = step * 3 * rows
        made_ref[pl.ds(at, rows), :] = row(12) + row(6) * field[0]
        made_ref[pl.ds(at + rows, rows), :] = row(7) * field[0] + row(8) * field[1]
        made_ref[pl.ds(at + 2 * rows, rows), :] = (
            row(9) * field[0] + row(10) * field[1] + row(11) * field[2]
        )
        copy = pltpu.make_async_copy(
            made_ref.at[pl.ds(at, 3 * rows)], velocity_ref.at[pl.ds(base + at, 3 * rows)],
            sems.at[step],
        )
        copy.start()
        copies.append(copy)
    return copies


def first_steps_kernel(
    mine_ref, theirs_ref, near_ref, weight_ref, row_ref, before_ref, velocity_ref, field_ref,
    made_ref, sems,
):
    for copy in some_steps(
        0, mine_ref, theirs_ref, near_ref, weight_ref, row_ref, before_ref, velocity_ref,
        made_ref, field_ref, sems,
    ):
        copy.wait()


def last_steps_kernel(
    _, mine_ref, theirs_ref, near_ref, weight_ref, row_ref, before_ref, velocity_ref, state_ref,
    made_ref, field_ref, sems,
):
    copies = some_steps(
        mine_ref.shape[0] - near_ref.shape[0], mine_ref, theirs_ref, near_ref, weight_ref,
        row_ref, before_ref, velocity_ref, made_ref, field_ref, sems,
    )
    copy = pltpu.make_async_copy(field_ref, state_ref, sems.at[len(copies)])
    copy.start()
    for one in copies + [copy]:
        one.wait()


WHOLE = pl.BlockSpec(memory_space=pltpu.VMEM)


def vmem(x):
    return pltpu.with_memory_space_constraint(x, pltpu.VMEM)


def hbm(x):
    return pltpu.with_memory_space_constraint(x, pltpu.HBM)


def call(kernel, out, scratch, flops, *args, in_specs=None, out_specs=None, **more):
    moved = sum(a.size * a.dtype.itemsize for a in args)
    return pl.pallas_call(
        kernel,
        out_shape=out,
        in_specs=in_specs or [WHOLE] * len(args),
        out_specs=out_specs or jax.tree.map(lambda _: WHOLE, out),
        scratch_shapes=scratch,
        cost_estimate=pl.CostEstimate(flops=flops, bytes_accessed=moved, transcendentals=0),
        compiler_params=pltpu.CompilerParams(vmem_limit_bytes=VMEM_BYTES),
        **more,
    )(*args)


def of_rows(scalars, rows):
    row = lax.broadcasted_iota(jnp.int32, (rows, LANES), 0)
    total = jnp.full((rows, LANES), scalars[0])
    for index in range(1, rows):
        total = jnp.where(row == index, scalars[index], total)
    return total


def weight_kernel(
    width_ref, other_ref, scale_ref, factor_ref, mean_ref, own_ref, far_ref, near_ref, row_ref
):
    rows = width_ref.shape[0]
    sign = 1 - 2 * (lax.axis_index("wall") % 2)
    lane = lax.broadcasted_iota(jnp.int32, (rows, LANES), 1)
    row = lax.broadcasted_iota(jnp.int32, (rows, LANES), 0)

    def raw(widths, offset):
        spread = widths.astype(f32)
        distance = offset.astype(f32)
        return jnp.where(
            jnp.abs(offset) <= widths,
            jnp.exp(-2.0 * math.pi * distance * distance / (spread * spread)),
            0.0,
        )

    def unit(widths, start):
        every = raw(widths, lane - HMAX)
        size = jnp.sqrt(jnp.sum(every * every, axis=1, keepdims=True))
        return raw(widths, lane % rows - row + start) / size

    def three(weights):
        high, low = halves(weights)
        return jnp.where(lane < 2 * rows, high.astype(f32), low.astype(f32))[:, : 3 * rows].astype(bf16)

    mine = of_rows([width_ref[i] for i in range(rows)], rows)
    other = of_rows([other_ref[i] for i in range(rows)], rows)
    own_ref[:rows, :] = three(unit(mine, 0))
    own_ref[rows:, :] = three(unit(other, -rows * sign))
    far_ref[:rows, :] = three(unit(mine, -rows * sign))
    far_ref[rows:, :] = three(unit(other, -2 * rows * sign))
    near_ref[...] = three(unit(mine, -2 * rows * sign))
    for part in range(3):
        scale = of_rows([scale_ref[part, i] for i in range(rows)], rows)
        row_ref[part] = jnp.exp(-math.pi / (2.0 * scale))
        row_ref[3 + part] = jnp.sqrt(1.0 - jnp.exp(-math.pi / scale))
    for entry in range(6):
        row_ref[6 + entry] = of_rows([factor_ref[entry, i] for i in range(rows)], rows)
    row_ref[12] = of_rows([mean_ref[i] for i in range(rows)], rows)


def planes(random_planes, previous, half_width, time_scale, lund_factor, mean_velocity):
    steps, parts, rows, width = random_planes.shape
    wall = lax.axis_size("wall")
    span = lax.axis_size("span")
    near_pairs = []
    far_pairs = []
    for at in range(wall):
        step = 1 - 2 * (at % 2)
        if 0 <= at - step < wall:
            far_pairs.append((at - step, at))
        if 0 <= at - 2 * step < wall:
            near_pairs.append((at - 2 * step, at))
    swap = [(at, at ^ 1) for at in range(wall)]
    forward = [(i, (i + 1) % span) for i in range(span)]
    backward = [(target, source) for source, target in forward]

    x = random_planes.reshape(steps * parts * rows, width)
    count = x.shape[0]
    packed_rows = count * EDGE // LANES
    far = lax.ppermute(x, "wall", far_pairs)
    packed = pltpu.VMEM((packed_rows, LANES), f32)
    mine_right, mine_left = call(
        pack_kernel, (packed, packed), [], 0, hbm(x), hbm(x),
        in_specs=[
            pl.BlockSpec((count, LANES), lambda i: (0, 0)),
            pl.BlockSpec((count, LANES), lambda i: (0, width // LANES - 1)),
        ],
        grid=(1,),
    )
    left = lax.ppermute(mine_left, "span", forward)
    right = lax.ppermute(mine_right, "span", backward)

    band = jnp.asarray(span_band())
    split = max(steps - LAST_STEPS, 1) * parts * rows
    block = pltpu.VMEM(x.shape, f32)
    part = pltpu.VMEM((count, width - 2 * TILE), f32)
    inner = [pltpu.VMEM((count, width - 2 * TILE + 2 * LANES), bf16)] * 2
    outer = [pltpu.VMEM((count, 2 * TILE + 4 * LANES), bf16)] * 2
    window = [pltpu.VMEM((count, width + 2 * LANES), bf16)] * 2
    far_parts = [pltpu.VMEM((count, width), bf16)] * 2
    span_flops = count * width * 512 * 3
    wall_flops = count * width * 32 * 6
    own, band = call(
        own_inner_kernel, (part, pltpu.VMEM(band.shape, bf16)),
        inner + [pltpu.SemaphoreType.DMA(())], span_flops, vmem(x), hbm(band),
        in_specs=[WHOLE, pl.BlockSpec(memory_space=pl.ANY)],
    )
    own_first, own_last, far_edges = call(
        own_outer_kernel,
        (
            pltpu.VMEM((split, width), f32), pltpu.VMEM((count - split, width), f32),
            pltpu.VMEM((2 * packed_rows, LANES), f32),
        ),
        outer, span_flops, vmem(own), vmem(x), vmem(left), vmem(right), vmem(band),
    )
    near_first = lax.ppermute(own_first, "wall", near_pairs)
    near_last = lax.ppermute(own_last, "wall", near_pairs)
    far_edges = lax.ppermute(far_edges, "wall", far_pairs)
    other_width = lax.ppermute(half_width, "wall", swap)

    scalars = pl.BlockSpec(memory_space=pltpu.SMEM)
    own_both, far_both, near_w, per_row = call(
        weight_kernel,
        (
            pltpu.VMEM((2 * rows, 3 * rows), bf16), pltpu.VMEM((2 * rows, 3 * rows), bf16),
            pltpu.VMEM((rows, 3 * rows), bf16), pltpu.VMEM((13, rows, LANES), f32),
        ),
        [], 0, half_width, other_width, time_scale, lund_factor, mean_velocity,
        in_specs=[scalars] * 5,
    )
    mine, theirs = call(
        own_sums_kernel, (block, block), [], wall_flops, vmem(own_first),
        vmem(own_last), vmem(own_both),
    )
    mine, theirs = call(
        far_sums_kernel, (block, block), window + far_parts,
        2 * span_flops + wall_flops, vmem(mine), vmem(theirs), vmem(far), vmem(far_edges),
        vmem(band), vmem(far_both),
    )
    theirs = lax.ppermute(theirs, "wall", swap)
    mine, theirs, near_w, per_row = vmem(mine), vmem(theirs), vmem(near_w), vmem(per_row)
    line = (parts * rows, width)
    anywhere = pl.BlockSpec(memory_space=pl.ANY)
    velocity, field = call(
        first_steps_kernel,
        (jax.ShapeDtypeStruct(x.shape, f32), pltpu.VMEM(line, f32)),
        [pltpu.VMEM((split, width), f32), pltpu.SemaphoreType.DMA((steps,))],
        wall_flops, mine, theirs, vmem(near_first), near_w, per_row,
        vmem(previous.reshape(line)), out_specs=(anywhere, WHOLE),
    )
    velocity, state = call(
        last_steps_kernel,
        (jax.ShapeDtypeStruct(x.shape, f32), jax.ShapeDtypeStruct(line, f32)),
        [
            pltpu.VMEM((count - split, width), f32), pltpu.VMEM(line, f32),
            pltpu.SemaphoreType.DMA((steps + 1,)),
        ],
        wall_flops, velocity, mine, theirs, vmem(near_last), near_w, per_row, vmem(field),
        in_specs=[anywhere] + [WHOLE] * 6, out_specs=(anywhere, anywhere),
        input_output_aliases={0: 0},
    )
    return velocity.reshape(random_planes.shape), state.reshape(previous.shape)


def solution(mesh):
    in_specs = (
        P(None, None, "wall", "span"),
        P(None, "wall", "span"),
        P("wall"),
        P(None, "wall"),
        P(None, "wall"),
        P("wall"),
    )
    out_specs = (P(None, None, "wall", "span"), P(None, "wall", "span"))
    return jax.shard_map(planes, mesh=mesh, in_specs=in_specs, out_specs=out_specs, check_vma=False)
```

```python
import math

import jax
import jax.numpy as jnp
import numpy as np
from jax import lax
from jax.experimental import pallas as pl
from jax.experimental.pallas import tpu as pltpu
from jax.sharding import PartitionSpec as P


HMAX = 32
HZ = 24
LANES = 128
TILE = 256
EDGE = HZ
LAST_STEPS = 2
VMEM_BYTES = 16 * 2**20

f32 = jnp.float32
bf16 = jnp.bfloat16


def span_band():
    offsets = np.arange(-HZ, HZ + 1, dtype=np.float64)
    raw = np.exp(-2.0 * np.pi * offsets**2 / HZ**2)
    unit = raw / np.sqrt(np.sum(raw * raw))
    rows = np.arange(TILE + 2 * LANES)[:, None]
    cols = np.arange(TILE)[None, :]
    j = rows - LANES - cols
    band = np.where(np.abs(j) <= HZ, unit[np.clip(j + HZ, 0, 2 * HZ)], 0.0).astype(np.float32)
    high = band.astype(jnp.bfloat16)
    low = (band - high.astype(np.float32)).astype(jnp.bfloat16)
    return np.stack([high, low])


def halves(x):
    high = x.astype(bf16)
    return high, (x - high.astype(f32)).astype(bf16)


def dot(a, b):
    return jnp.dot(a, b, preferred_element_type=f32)


def spread(packed, last, count):
    pieces = []
    for group in range(LANES // EDGE):
        shift = (LANES - EDGE if last else 0) - group * EDGE
        pieces.append(pltpu.roll(packed, shift % LANES, 1) if shift else packed)
    return jnp.concatenate(pieces, axis=0)[:count]


def gathered(edge, last, count):
    lane = lax.broadcasted_iota(jnp.int32, (count, LANES), 1)
    total = jnp.zeros((count, LANES), f32)
    for group in range(LANES // EDGE):
        piece = edge[group * count : (group + 1) * count]
        if piece.shape[0] < count:
            fill = jnp.zeros((count - piece.shape[0], LANES), f32)
            piece = jnp.concatenate([piece, fill], axis=0)
        shift = group * EDGE - (LANES - EDGE if last else 0)
        here = (lane >= group * EDGE) & (lane < (group + 1) * EDGE)
        total = jnp.where(here, pltpu.roll(piece, shift % LANES, 1) if shift else piece, total)
    return total


def pack_kernel(first_ref, last_ref, right_ref, left_ref):
    right_ref[...] = gathered(first_ref[...], False, right_ref.shape[0])
    left_ref[...] = gathered(last_ref[...], True, left_ref.shape[0])


def put(high_ref, low_ref, start, value):
    at = pl.ds(start, value.shape[1])
    high_ref[:, at], low_ref[:, at] = halves(value)


def fill_inner(x_ref, high_ref, low_ref):
    width = x_ref.shape[1]
    put(high_ref, low_ref, 0, x_ref[:, TILE - LANES : width - TILE + LANES])


def fill_outer(x_ref, left, right, high_ref, low_ref):
    own = TILE + LANES
    put(high_ref, low_ref, 0, spread(left, True, x_ref.shape[0]))
    put(high_ref, low_ref, LANES, x_ref[:, :own])
    put(high_ref, low_ref, LANES + own, x_ref[:, x_ref.shape[1] - own :])
    put(high_ref, low_ref, LANES + 2 * own, spread(right, False, x_ref.shape[0]))


def filtered(high_ref, low_ref, band_ref, start):
    window = pl.ds(start, TILE + 2 * LANES)
    high = high_ref[:, window]
    return (
        dot(high, band_ref[0]) + dot(low_ref[:, window], band_ref[0]) + dot(high, band_ref[1])
    )


def own_inner_kernel(x_ref, band_hbm, out_ref, band_ref, high_ref, low_ref, sem):
    copy = pltpu.make_async_copy(band_hbm, band_ref, sem)
    copy.start()
    fill_inner(x_ref, high_ref, low_ref)
    copy.wait()
    for at in range(TILE, x_ref.shape[1] - TILE, TILE):
        out_ref[:, at - TILE : at] = filtered(high_ref, low_ref, band_ref, at - TILE)


def own_outer_kernel(
    inner_ref, x_ref, left_ref, right_ref, band_ref, first_ref, last_ref, edge_ref,
    high_ref, low_ref,
):
    count = left_ref.shape[0]
    edge_ref[:count, :] = left_ref[...]
    edge_ref[count:, :] = right_ref[...]
    fill_outer(x_ref, left_ref[...], right_ref[...], high_ref, low_ref)
    split = first_ref.shape[0]
    end = x_ref.shape[1] - TILE
    first_ref[:, TILE:end] = inner_ref[:split, :]
    last_ref[:, TILE:end] = inner_ref[split:, :]
    for at, start in ((0, 0), (end, TILE + 2 * LANES)):
        value = filtered(high_ref, low_ref, band_ref, start)
        first_ref[:, at : at + TILE] = value[:split]
        last_ref[:, at : at + TILE] = value[split:]


def wall_sums(block_of, weight_ref, planes, store):
    rows = weight_ref.shape[0] // 2
    group = 6

    def some_planes(index, carry):
        for one in range(group):
            at = pl.ds(pl.multiple_of((index * group + one) * rows, rows), rows)
            high, low = block_of(at)
            both = dot(weight_ref[...], jnp.concatenate([high, low, high], axis=0))
            store(at, both[:rows], both[rows:])
        return carry

    lax.fori_loop(0, planes // group, some_planes, 0)


def own_sums_kernel(first_ref, last_ref, weight_ref, mine_ref, theirs_ref):
    rows = weight_ref.shape[0] // 2
    base = 0
    for own_ref in (first_ref, last_ref):

        def store(at, mine, theirs, base=base):
            to = pl.ds(pl.multiple_of(at.start + base, rows), rows)
            mine_ref[to, :] = mine
            theirs_ref[to, :] = theirs

        planes = own_ref.shape[0] // rows
        wall_sums(lambda at, own_ref=own_ref: halves(own_ref[at, :]), weight_ref, planes, store)
        base += own_ref.shape[0]


def far_sums_kernel(
    mine_own_ref, theirs_own_ref, far_ref, edge_ref, band_ref, weight_ref, mine_ref, theirs_ref,
    high_ref, low_ref, far_high_ref, far_low_ref,
):
    count = edge_ref.shape[0] // 2
    width = far_ref.shape[1]
    put(high_ref, low_ref, 0, spread(edge_ref[:count, :], True, far_ref.shape[0]))
    put(high_ref, low_ref, LANES, far_ref[...])
    put(high_ref, low_ref, LANES + width, spread(edge_ref[count:, :], False, far_ref.shape[0]))
    for at in range(0, width, TILE):
        put(far_high_ref, far_low_ref, at, filtered(high_ref, low_ref, band_ref, at))

    def store(at, mine, theirs):
        mine_ref[at, :] = mine_own_ref[at, :] + mine
        theirs_ref[at, :] = theirs_own_ref[at, :] + theirs

    planes = far_ref.shape[0] * 2 // weight_ref.shape[0]
    wall_sums(lambda at: (far_high_ref[at, :], far_low_ref[at, :]), weight_ref, planes, store)


def some_steps(
    base, mine_ref, theirs_ref, near_ref, weight_ref, row_ref, before_ref, velocity_ref,
    state_ref, made_ref, field_ref, sems,
):
    rows = weight_ref.shape[0]
    repeat = near_ref.shape[1] // LANES

    def row(index):
        return jnp.concatenate([row_ref[index]] * repeat, axis=1)

    copies = []

    def send(source, target):
        copy = pltpu.make_async_copy(source, target, sems.at[len(copies)])
        copy.start()
        copies.append(copy)

    def made(at, value):
        made_ref[pl.ds(at, rows), :] = value
        send(made_ref.at[pl.ds(at, rows)], velocity_ref.at[pl.ds(base + at, rows)])

    steps = near_ref.shape[0] // (3 * rows)
    for step in range(steps):
        field = []
        start = step * 3 * rows
        for part in range(3):
            at = start + part * rows
            of = pl.ds(part * rows, rows)
            high, low = halves(near_ref[pl.ds(at, rows), :])
            total = mine_ref[pl.ds(base + at, rows), :] + theirs_ref[pl.ds(base + at, rows), :]
            total = total + dot(weight_ref[...], jnp.concatenate([high, low, high], axis=0))
            before = before_ref[of, :] if step == 0 else field_ref[of, :]
            now = row(part) * before + row(3 + part) * total
            field_ref[of, :] = now
            field.append(now)
            if state_ref is not None and step == steps - 1:
                send(field_ref.at[of], state_ref.at[of])
            if part == 0:
                made(at, row(12) + row(6) * field[0])
            elif part == 1:
                made(at, row(7) * field[0] + row(8) * field[1])
            else:
                made(at, row(9) * field[0] + row(10) * field[1] + row(11) * field[2])
    for copy in copies:
        copy.wait()


def first_steps_kernel(
    mine_ref, theirs_ref, near_ref, weight_ref, row_ref, before_ref, velocity_ref, field_ref,
    made_ref, sems,
):
    some_steps(
        0, mine_ref, theirs_ref, near_ref, weight_ref, row_ref, before_ref, velocity_ref,
        None, made_ref, field_ref, sems,
    )


def last_steps_kernel(
    _, mine_ref, theirs_ref, near_ref, weight_ref, row_ref, before_ref, velocity_ref, state_ref,
    made_ref, field_ref, sems,
):
    some_steps(
        mine_ref.shape[0] - near_ref.shape[0], mine_ref, theirs_ref, near_ref, weight_ref,
        row_ref, before_ref, velocity_ref, state_ref, made_ref, field_ref, sems,
    )


WHOLE = pl.BlockSpec(memory_space=pltpu.VMEM)


def vmem(x):
    return pltpu.with_memory_space_constraint(x, pltpu.VMEM)


def hbm(x):
    return pltpu.with_memory_space_constraint(x, pltpu.HBM)


def call(kernel, out, scratch, flops, *args, in_specs=None, out_specs=None, **more):
    moved = sum(a.size * a.dtype.itemsize for a in args)
    return pl.pallas_call(
        kernel,
        out_shape=out,
        in_specs=in_specs or [WHOLE] * len(args),
        out_specs=out_specs or jax.tree.map(lambda _: WHOLE, out),
        scratch_shapes=scratch,
        cost_estimate=pl.CostEstimate(flops=flops, bytes_accessed=moved, transcendentals=0),
        compiler_params=pltpu.CompilerParams(vmem_limit_bytes=VMEM_BYTES),
        **more,
    )(*args)


def of_rows(scalars, rows):
    row = lax.broadcasted_iota(jnp.int32, (rows, LANES), 0)
    total = jnp.full((rows, LANES), scalars[0])
    for index in range(1, rows):
        total = jnp.where(row == index, scalars[index], total)
    return total


def weight_kernel(
    width_ref, other_ref, scale_ref, factor_ref, mean_ref, own_ref, far_ref, near_ref, row_ref
):
    rows = width_ref.shape[0]
    sign = 1 - 2 * (lax.axis_index("wall") % 2)
    lane = lax.broadcasted_iota(jnp.int32, (rows, LANES), 1)
    row = lax.broadcasted_iota(jnp.int32, (rows, LANES), 0)

    def raw(widths, offset):
        spread = widths.astype(f32)
        distance = offset.astype(f32)
        return jnp.where(
            jnp.abs(offset) <= widths,
            jnp.exp(-2.0 * math.pi * distance * distance / (spread * spread)),
            0.0,
        )

    def unit(widths, start):
        every = raw(widths, lane - HMAX)
        size = jnp.sqrt(jnp.sum(every * every, axis=1, keepdims=True))
        return raw(widths, lane % rows - row + start) / size

    def three(weights):
        high, low = halves(weights)
        return jnp.where(lane < 2 * rows, high.astype(f32), low.astype(f32))[:, : 3 * rows].astype(bf16)

    mine = of_rows([width_ref[i] for i in range(rows)], rows)
    other = of_rows([other_ref[i] for i in range(rows)], rows)
    own_ref[:rows, :] = three(unit(mine, 0))
    own_ref[rows:, :] = three(unit(other, -rows * sign))
    far_ref[:rows, :] = three(unit(mine, -rows * sign))
    far_ref[rows:, :] = three(unit(other, -2 * rows * sign))
    near_ref[...] = three(unit(mine, -2 * rows * sign))
    for part in range(3):
        scale = of_rows([scale_ref[part, i] for i in range(rows)], rows)
        row_ref[part] = jnp.exp(-math.pi / (2.0 * scale))
        row_ref[3 + part] = jnp.sqrt(1.0 - jnp.exp(-math.pi / scale))
    for entry in range(6):
        row_ref[6 + entry] = of_rows([factor_ref[entry, i] for i in range(rows)], rows)
    row_ref[12] = of_rows([mean_ref[i] for i in range(rows)], rows)


def planes(random_planes, previous, half_width, time_scale, lund_factor, mean_velocity):
    steps, parts, rows, width = random_planes.shape
    wall = lax.axis_size("wall")
    span = lax.axis_size("span")
    near_pairs = []
    far_pairs = []
    for at in range(wall):
        step = 1 - 2 * (at % 2)
        if 0 <= at - step < wall:
            far_pairs.append((at - step, at))
        if 0 <= at - 2 * step < wall:
            near_pairs.append((at - 2 * step, at))
    swap = [(at, at ^ 1) for at in range(wall)]
    forward = [(i, (i + 1) % span) for i in range(span)]
    backward = [(target, source) for source, target in forward]

    x = random_planes.reshape(steps * parts * rows, width)
    count = x.shape[0]
    packed_rows = -(-count // (8 * (LANES // EDGE))) * 8
    far = lax.ppermute(x, "wall", far_pairs)
    packed = pltpu.VMEM((packed_rows, LANES), f32)
    mine_right, mine_left = call(
        pack_kernel, (packed, packed), [], 0, hbm(x), hbm(x),
        in_specs=[
            pl.BlockSpec((count, LANES), lambda i: (0, 0)),
            pl.BlockSpec((count, LANES), lambda i: (0, width // LANES - 1)),
        ],
        grid=(1,),
    )
    left = lax.ppermute(mine_left, "span", forward)
    right = lax.ppermute(mine_right, "span", backward)

    band = jnp.asarray(span_band())
    split = max(steps - LAST_STEPS, 1) * parts * rows
    block = pltpu.VMEM(x.shape, f32)
    part = pltpu.VMEM((count, width - 2 * TILE), f32)
    inner = [pltpu.VMEM((count, width - 2 * TILE + 2 * LANES), bf16)] * 2
    outer = [pltpu.VMEM((count, 2 * TILE + 4 * LANES), bf16)] * 2
    window = [pltpu.VMEM((count, width + 2 * LANES), bf16)] * 2
    far_parts = [pltpu.VMEM((count, width), bf16)] * 2
    span_flops = count * width * 512 * 3
    wall_flops = count * width * 32 * 6
    own, band = call(
        own_inner_kernel, (part, pltpu.VMEM(band.shape, bf16)),
        inner + [pltpu.SemaphoreType.DMA(())], span_flops, vmem(x), hbm(band),
        in_specs=[WHOLE, pl.BlockSpec(memory_space=pl.ANY)],
    )
    own_first, own_last, far_edges = call(
        own_outer_kernel,
        (
            pltpu.VMEM((split, width), f32), pltpu.VMEM((count - split, width), f32),
            pltpu.VMEM((2 * packed_rows, LANES), f32),
        ),
        outer, span_flops, vmem(own), vmem(x), vmem(left), vmem(right), vmem(band),
    )
    near_first = lax.ppermute(own_first, "wall", near_pairs)
    near_last = lax.ppermute(own_last, "wall", near_pairs)
    far_edges = lax.ppermute(far_edges, "wall", far_pairs)
    other_width = lax.ppermute(half_width, "wall", swap)

    scalars = pl.BlockSpec(memory_space=pltpu.SMEM)
    own_both, far_both, near_w, per_row = call(
        weight_kernel,
        (
            pltpu.VMEM((2 * rows, 3 * rows), bf16), pltpu.VMEM((2 * rows, 3 * rows), bf16),
            pltpu.VMEM((rows, 3 * rows), bf16), pltpu.VMEM((13, rows, LANES), f32),
        ),
        [], 0, half_width, other_width, time_scale, lund_factor, mean_velocity,
        in_specs=[scalars] * 5,
    )
    mine, theirs = call(
        own_sums_kernel, (block, block), [], wall_flops, vmem(own_first),
        vmem(own_last), vmem(own_both),
    )
    mine, theirs = call(
        far_sums_kernel, (block, block), window + far_parts,
        2 * span_flops + wall_flops, vmem(mine), vmem(theirs), vmem(far), vmem(far_edges),
        vmem(band), vmem(far_both),
    )
    theirs = lax.ppermute(theirs, "wall", swap)
    mine, theirs, near_w, per_row = vmem(mine), vmem(theirs), vmem(near_w), vmem(per_row)
    line = (parts * rows, width)
    anywhere = pl.BlockSpec(memory_space=pl.ANY)
    velocity, field = call(
        first_steps_kernel,
        (jax.ShapeDtypeStruct(x.shape, f32), pltpu.VMEM(line, f32)),
        [pltpu.VMEM((split, width), f32), pltpu.SemaphoreType.DMA((3 * steps,))],
        wall_flops, mine, theirs, vmem(near_first), near_w, per_row,
        vmem(previous.reshape(line)), out_specs=(anywhere, WHOLE),
    )
    velocity, state = call(
        last_steps_kernel,
        (jax.ShapeDtypeStruct(x.shape, f32), jax.ShapeDtypeStruct(line, f32)),
        [
            pltpu.VMEM((count - split, width), f32), pltpu.VMEM(line, f32),
            pltpu.SemaphoreType.DMA((3 * steps + 3,)),
        ],
        wall_flops, velocity, mine, theirs, vmem(near_last), near_w, per_row, vmem(field),
        in_specs=[anywhere] + [WHOLE] * 6, out_specs=(anywhere, anywhere),
        input_output_aliases={0: 0},
    )
    return velocity.reshape(random_planes.shape), state.reshape(previous.shape)


def solution(mesh):
    in_specs = (
        P(None, None, "wall", "span"),
        P(None, "wall", "span"),
        P("wall"),
        P(None, "wall"),
        P(None, "wall"),
        P("wall"),
    )
    out_specs = (P(None, None, "wall", "span"), P(None, "wall", "span"))
    return jax.shard_map(planes, mesh=mesh, in_specs=in_specs, out_specs=out_specs, check_vma=False)
```
